32 devices in a mesh: groups: 2 (over x), ref: 16 (over z, y, core).
Axes of the slice: x: 2, y: 2, z: 4, core: 2. Of those that a mesh axis runs over, the one named last changes fastest.
Arguments:
- long_series: bfloat16 [131072], P(('groups', 'ref')), parts along dimension 0, may hold values from -12 to 12
- queries: bfloat16 [64, 1024], P(('groups', 'ref')), parts along dimension 0, may hold values from -48 to 48
- lengths: int32 [64], P(('groups', 'ref')), parts along dimension 0, may hold values from 512 to 1024, as said below
- groups: int32 [64], P(('groups', 'ref')), parts along dimension 0, may hold values from 0 to 15, as said below
Outputs:
- profile: float32 [64, 1024], P(('groups', 'ref')), parts along dimension 0
The draws below stay inside these ranges and needn't reach their ends.
There are 2 independent parts, one for each index of `groups`. The reference program is written for one: setup_inputs(seed, part) draws one part's arguments, and reference() takes and returns one part's arrays. A program takes and returns all parts, laid end to end along the dimension named above; each array names one. Nothing has to cross between parts.
Inputs may be any that keep to these rules, and one draw needn't show every extreme that they name: `lengths`: multiples of 128. `groups`: region g holds reference blocks g * 1 to (g + 1) * 1 - 1; at most 4 queries name one region, and one region is named by exactly 4.
All inputs are finite; a program needn't handle non-finite values.
Results may differ from the reference program's by a relative error of at most 0.0003.
Values may be sent and summed in bfloat16 or wider, within the bound.
A program may use at most 64 MiB of HBM per device.

```python
import math
import jax
import jax.numpy as jnp
from jax import lax

M = 256
LQ = 1024
RDEV = 4096
GDEV = 1
RMAX = 4
NQ = 32
NR = 65536
NGRP = 16


def make_join(key):
    blocks = NR // 128
    values = jax.random.normal(jax.random.fold_in(key, 1), (NR,), jnp.float32)
    shifts = 0.5 * jax.random.normal(jax.random.fold_in(key, 2), (blocks,), jnp.float32)
    scales = jnp.exp(jax.random.uniform(jax.random.fold_in(key, 3), (blocks,), jnp.float32, math.log(0.5), math.log(2.0)))
    series = jnp.clip(values * jnp.repeat(scales, 128) + jnp.repeat(shifts, 128), -12.0, 12.0)
    order = jax.random.permutation(jax.random.fold_in(key, 4), NQ)
    position = jnp.argsort(order)
    leader = jax.random.randint(jax.random.fold_in(key, 5), (), 0, NGRP)
    others = (leader + 1 + (position - RMAX) % (NGRP - 1)) % NGRP
    groups = jnp.where(position < RMAX, leader, others).astype(jnp.int32)
    copies = LQ // M
    starts = groups[:, None] * (GDEV * RDEV) + jax.random.randint(jax.random.fold_in(key, 6), (NQ, copies), 0, GDEV * RDEV - M + 1)
    gather_index = (starts[:, :, None] + jnp.arange(M, dtype=jnp.int32)[None, None, :]).reshape(NQ, LQ)
    copied = series[gather_index]
    noise_level = jnp.exp(jax.random.uniform(jax.random.fold_in(key, 7), (NQ, LQ // 128), jnp.float32, math.log(0.05), math.log(3.0)))
    noise = jax.random.normal(jax.random.fold_in(key, 8), (NQ, LQ), jnp.float32)
    made = copied + jnp.repeat(noise_level, 128, axis=1) * noise
    return (series, jnp.clip(made, -48.0, 48.0), groups)


def draw_long_series(key, part):
    return make_join(key)[0].astype(jnp.bfloat16)


def draw_queries(key, part):
    return make_join(key)[1].astype(jnp.bfloat16)


def draw_groups(key, part):
    return make_join(key)[2]


def draw_lengths(key, part):
    units = jax.random.randint(jax.random.fold_in(key, 31), (NQ,), LQ // 256, LQ // 128 + 1)
    sized = 128 * units
    return sized.at[0].set(LQ).at[1].set(LQ // 2).astype(jnp.int32)


def setup_inputs(seed: int = 0, part: int = 0) -> dict:
    keys = jax.random.split(jax.random.key(seed), 5)
    own_keys = jax.random.split(jax.random.fold_in(keys[4], part), 5)
    long_series = draw_long_series(jax.random.fold_in(jax.random.fold_in(keys[4], part), 71), part)
    queries = draw_queries(jax.random.fold_in(jax.random.fold_in(keys[4], part), 71), part)
    lengths = draw_lengths(jax.random.fold_in(jax.random.fold_in(keys[4], part), 71), part)
    groups = draw_groups(jax.random.fold_in(jax.random.fold_in(keys[4], part), 71), part)
    return dict(long_series=long_series, queries=queries, lengths=lengths, groups=groups)


SPREAD_FLOOR = 0.25

def window_stats(series, count):
    offsets_grid = jnp.arange(count, dtype=jnp.int32)[:, None] + jnp.arange(M, dtype=jnp.int32)[None, :]
    windows = series[offsets_grid]
    values = windows.astype(jnp.float32)
    centre = lax.optimization_barrier(jnp.mean(values, axis=1))
    spread = jnp.sqrt(lax.optimization_barrier(jnp.mean((values - centre[:, None]) ** 2, axis=1)) + SPREAD_FLOOR)
    return (windows, centre, spread)

def best_match(query_set, ref_set, usable):
    query_windows, query_centre, query_spread = query_set
    ref_windows, ref_centre, ref_spread = ref_set
    products = lax.dot_general(query_windows.astype(jnp.float32), ref_windows.astype(jnp.float32), (((1,), (1,)), ((), ())), precision=lax.Precision.HIGHEST, preferred_element_type=jnp.float32)
    correlation = (products - M * query_centre[:, None] * ref_centre[None, :]) / (M * query_spread[:, None] * ref_spread[None, :])
    correlation = jnp.where(usable[None, :], correlation, -2.0)
    return lax.optimization_barrier(jnp.max(correlation, axis=1))

def reference(long_series, queries, lengths, groups):
    overall = long_series.shape[0]
    padded = jnp.concatenate([long_series, jnp.zeros((M,), jnp.bfloat16)])

    def match_query(entry_pair):
        series, region = entry_pair
        query_set = window_stats(jnp.concatenate([series, jnp.zeros((M,), jnp.bfloat16)]), LQ)
        best_so_far = jnp.full((LQ,), -2.0, jnp.float32)
        for offset in range(GDEV):
            block_index = region * GDEV + offset
            first_cell = (block_index * RDEV).astype(jnp.int32)
            segment = lax.dynamic_slice_in_dim(padded, first_cell, RDEV + M)
            ref_set = window_stats(segment, RDEV)
            usable = first_cell + jnp.arange(RDEV, dtype=jnp.int32) <= overall - M
            best_so_far = jnp.maximum(best_so_far, best_match(query_set, ref_set, usable))
        return best_so_far
    best_values = lax.map(match_query, (queries, groups))
    live_points = jnp.arange(LQ, dtype=jnp.int32)[None, :] <= lengths[:, None] - M
    return jnp.where(live_points, 2.0 * (1.0 - best_values), 0.0)
```

```python
import functools

import jax
import jax.numpy as jnp
from jax import lax
from jax.experimental import pallas as pl
from jax.experimental.pallas import tpu as pltpu
from jax.sharding import PartitionSpec as P

M = 256
LANES = 128
HALVES = M // LANES
SPREAD_FLOOR = 0.25
CHUNK = 4
MASKED = -1e30


def hankel(row, following):
    shape = (LANES, LANES)
    lane = lax.broadcasted_iota(jnp.int32, shape, 1)
    sub = lax.broadcasted_iota(jnp.int32, shape, 0)
    here = pltpu.roll(jnp.broadcast_to(row, shape), 1, 1, stride=1, stride_axis=0)
    there = pltpu.roll(jnp.broadcast_to(following, shape), 1, 1, stride=1, stride_axis=0)
    return jnp.where(lane <= sub, here, there)


def toeplitz(row, following):
    shape = (LANES, LANES)
    lane = lax.broadcasted_iota(jnp.int32, shape, 1)
    sub = lax.broadcasted_iota(jnp.int32, shape, 0)
    here = pltpu.roll(jnp.broadcast_to(row, shape), 0, 1, stride=1, stride_axis=0)
    there = pltpu.roll(jnp.broadcast_to(following, shape), 0, 1, stride=1, stride_axis=0)
    return jnp.where(lane >= sub, here, there)


def next_row(x):
    return pltpu.roll(x, x.shape[0] - 1, 0)


def window_stats(x):
    lane = lax.broadcasted_iota(jnp.int32, x.shape, 1)
    total, square = x, jnp.zeros_like(x)
    count = 1
    while count < M:
        def ahead(v):
            if count == LANES:
                return next_row(v)
            rolled = pltpu.roll(v, LANES - count, 1)
            return jnp.where(lane < LANES - count, rolled, next_row(rolled))

        total_ahead, square_ahead = ahead(total), ahead(square)
        gap = total - total_ahead
        square = square + square_ahead + gap * gap * (0.5 / count)
        total = total + total_ahead
        count *= 2
    return total, 1.0 / jnp.sqrt(square * (1.0 / M) + SPREAD_FLOOR)


def join_kernel(members, groups_ref, lengths_ref, q_ref, series_ref, out_ref,
                left_ref, right_ref, mean_ref, total_ref, scale_ref, acc_ref):
    per_device, series_len = q_ref.shape
    q_rows = series_len // LANES
    all_rows = series_ref.shape[0]
    rows = all_rows // members
    full = (series_len - M) // LANES
    tall = full * LANES + 16
    r_pad = rows + 8
    q_pad = q_rows + 8

    flip = (
        lax.broadcasted_iota(jnp.int32, (LANES, LANES), 0)
        + lax.broadcasted_iota(jnp.int32, (LANES, LANES), 1)
        == LANES - 1
    ).astype(jnp.bfloat16)

    parts = []
    for p in range(per_device):
        g = groups_ref[p]
        own = series_ref[pl.ds(pl.multiple_of(g * rows, rows), rows), :].astype(jnp.float32)
        after = jnp.minimum((g + 1) * rows, all_rows - 16)
        extra = series_ref[pl.ds(pl.multiple_of(after, 16), 16), :].astype(jnp.float32)[:8]
        parts += [own, jnp.where(g == members - 1, 0.0, extra)]
    q_all = q_ref[...].astype(jnp.float32)
    for p in range(per_device):
        pieces = [q_all[p : p + 1, LANES * a : LANES * (a + 1)] for a in range(q_rows)]
        parts += pieces + [jnp.zeros((q_pad - q_rows, LANES), jnp.float32)]
    points = jnp.concatenate(parts, axis=0)
    total, scale = window_stats(points)
    total_ref[...] = total
    scale_ref[...] = scale

    for p in range(per_device):
        r_base = p * r_pad
        q_base = per_device * r_pad + p * q_pad
        q_back = jnp.dot(
            points[q_base : q_base + q_pad].astype(jnp.bfloat16), flip, preferred_element_type=jnp.float32
        )
        for a in range(full + HALVES):
            tile = toeplitz(q_back[a : a + 1], q_back[a + 1 : a + 2]).astype(jnp.bfloat16)
            for h in range(HALVES):
                if 0 <= a - h < full:
                    left_ref[pl.ds((a - h) * LANES, LANES), pl.ds(h * LANES, LANES)] = tile
                elif a - h == full:
                    left_ref[pl.ds(full * LANES, 16), pl.ds(h * LANES, LANES)] = tile[:16]
        for m in range(rows + 1):
            right_ref[m] = hankel(
                points[r_base + m : r_base + m + 1], points[r_base + m + 1 : r_base + m + 2]
            ).astype(jnp.bfloat16)
        mean_ref[...] = jnp.dot(
            left_ref[...], jnp.full((M, LANES), 1.0 / M, jnp.bfloat16), preferred_element_type=jnp.float32
        )

        g = groups_ref[p]

        def chunk(first, last):
            right = jnp.concatenate(
                [
                    jnp.concatenate([right_ref[first + h + n] for n in range(CHUNK)], axis=1)
                    for h in range(HALVES)
                ],
                axis=0,
            )
            products = jnp.dot(left_ref[...], right, preferred_element_type=jnp.float32)
            totals = [total_ref[pl.ds(r_base + first + n, 1), :] for n in range(CHUNK)]
            scales = [scale_ref[pl.ds(r_base + first + n, 1), :] for n in range(CHUNK)]
            if last:
                lane = lax.broadcasted_iota(jnp.int32, (1, LANES), 1)
                start = (g * rows + first) * LANES
                limit = all_rows * LANES - M
                floors = [
                    jnp.where(start + n * LANES + lane <= limit, 0.0, MASKED) for n in range(CHUNK)
                ]
            for t in range(0, tall, 16):
                mean = mean_ref[pl.ds(t, 16), :]
                best = None
                for n in range(CHUNK):
                    piece = products[t : t + 16, n * LANES : (n + 1) * LANES]
                    value = (piece - mean * totals[n]) * scales[n]
                    if last:
                        value = value + floors[n]
                    best = value if best is None else jnp.maximum(best, value)
                if not last:
                    best = jnp.maximum(best, acc_ref[pl.ds(t, 16), :])
                acc_ref[pl.ds(t, 16), :] = best

        chunk(rows - CHUNK, True)

        @pl.loop(0, rows // CHUNK - 1)
        def _(c):
            chunk(c * CHUNK, False)

        lane = lax.broadcasted_iota(jnp.int32, (1, LANES), 1)
        limit = lengths_ref[p] - M
        for a in range(q_rows):
            if a < full:
                block = acc_ref[pl.ds(a * LANES, LANES), :]
                best = jnp.max(block.T, axis=0, keepdims=True)
            elif a == full:
                block = acc_ref[pl.ds(a * LANES, 8), :]
                best = jnp.broadcast_to(jnp.max(block, axis=1, keepdims=True)[:1], (1, LANES))
            if a <= full:
                best = best * scale_ref[pl.ds(q_base + a, 1), :] * (1.0 / M)
                row = jnp.where(a * LANES + lane <= limit, 2.0 * (1.0 - best), 0.0)
            else:
                row = jnp.zeros((1, LANES), jnp.float32)
            out_ref[pl.ds(p, 1), pl.ds(a * LANES, LANES)] = row


def join(members, groups, lengths, queries, series):
    per_device, series_len = queries.shape
    rows = series.shape[0] // members
    tall = (series_len - M) // LANES * LANES + 16
    stat_rows = per_device * (rows + 8 + series_len // LANES + 8)
    vmem = pl.BlockSpec(memory_space=pltpu.VMEM)
    smem = pl.BlockSpec(memory_space=pltpu.SMEM)
    return pl.pallas_call(
        functools.partial(join_kernel, members),
        out_shape=jax.ShapeDtypeStruct((per_device, series_len), jnp.float32),
        in_specs=[smem, smem, vmem, vmem],
        out_specs=vmem,
        scratch_shapes=[
            pltpu.VMEM((tall, M), jnp.bfloat16),
            pltpu.VMEM((rows + 1, LANES, LANES), jnp.bfloat16),
            pltpu.VMEM((tall, LANES), jnp.float32),
            pltpu.VMEM((stat_rows, LANES), jnp.float32),
            pltpu.VMEM((stat_rows, LANES), jnp.float32),
            pltpu.VMEM((tall, LANES), jnp.float32),
        ],
        name="join",
    )(groups, lengths, queries, series)


def body(long_series, queries, lengths, groups):
    members = lax.axis_size("ref")
    block = long_series.reshape(-1, LANES)
    series = lax.all_gather(block, "ref", axis=0, tiled=True)
    return join(members, groups, lengths, queries, series)


def solution(mesh):
    in_specs = (
        P(("groups", "ref")),
        P(("groups", "ref"), None),
        P(("groups", "ref")),
        P(("groups", "ref")),
    )
    out_specs = P(("groups", "ref"), None)
    return jax.shard_map(body, mesh=mesh, in_specs=in_specs, out_specs=out_specs, check_vma=False)
```

```python
import functools

import jax
import jax.numpy as jnp
from jax import lax
from jax.experimental import pallas as pl
from jax.experimental.pallas import tpu as pltpu
from jax.sharding import PartitionSpec as P

M = 256
LANES = 128
HALVES = M // LANES
SPREAD_FLOOR = 0.25
CHUNK = 4
MASKED = -1e30


def hankel(row, following):
    shape = (LANES, LANES)
    lane = lax.broadcasted_iota(jnp.int32, shape, 1)
    sub = lax.broadcasted_iota(jnp.int32, shape, 0)
    here = pltpu.roll(jnp.broadcast_to(row, shape), 1, 1, stride=1, stride_axis=0)
    there = pltpu.roll(jnp.broadcast_to(following, shape), 1, 1, stride=1, stride_axis=0)
    return jnp.where(lane <= sub, here, there)


def toeplitz(row, following):
    shape = (LANES, LANES)
    lane = lax.broadcasted_iota(jnp.int32, shape, 1)
    sub = lax.broadcasted_iota(jnp.int32, shape, 0)
    here = pltpu.roll(jnp.broadcast_to(row, shape), 0, 1, stride=1, stride_axis=0)
    there = pltpu.roll(jnp.broadcast_to(following, shape), 0, 1, stride=1, stride_axis=0)
    return jnp.where(lane >= sub, here, there)


def next_row(x):
    return pltpu.roll(x, x.shape[0] - 1, 0)


def window_stats(x):
    lane = lax.broadcasted_iota(jnp.int32, x.shape, 1)
    total, square = x, jnp.zeros_like(x)
    count = 1
    while count < M:
        def ahead(v):
            if count == LANES:
                return next_row(v)
            rolled = pltpu.roll(v, LANES - count, 1)
            return jnp.where(lane < LANES - count, rolled, next_row(rolled))

        total_ahead, square_ahead = ahead(total), ahead(square)
        gap = total - total_ahead
        square = square + square_ahead + gap * gap * (0.5 / count)
        total = total + total_ahead
        count *= 2
    return total, 1.0 / jnp.sqrt(square * (1.0 / M) + SPREAD_FLOOR)


def to_peers(members, block_ref, series_ref, send_sem, recv_sem, arriving):
    rows = block_ref.shape[0]
    me = lax.axis_index("ref")

    def copy(d):
        owner = lax.rem(me + members - d, members) if arriving else me
        return pltpu.make_async_remote_copy(
            src_ref=block_ref,
            dst_ref=series_ref.at[pl.ds(pl.multiple_of(owner * rows, rows), rows), :],
            send_sem=send_sem.at[d],
            recv_sem=recv_sem.at[d],
            device_id={"ref": lax.rem(me + d, members)},
            device_id_type=pl.DeviceIdType.MESH,
        )

    return copy


def join_kernel(members, groups_ref, lengths_ref, q_ref, block_ref, out_ref,
                series_ref, left_ref, right_ref, mean_ref, total_ref, scale_ref, q_scale_ref, acc_ref,
                send_sem, recv_sem):
    per_device, series_len = q_ref.shape
    q_rows = series_len // LANES
    rows = block_ref.shape[0]
    all_rows = series_ref.shape[0]
    full = (series_len - M) // LANES
    tall = full * LANES + 16
    r_pad = rows + 8
    q_pad = q_rows + 8
    me = lax.axis_index("ref")

    barrier = pltpu.get_barrier_semaphore()

    @pl.loop(1, members)
    def _(d):
        pl.semaphore_signal(
            barrier, inc=1, device_id={"ref": lax.rem(me + d, members)}, device_id_type=pl.DeviceIdType.MESH
        )

    series_ref[pl.ds(pl.multiple_of(me * rows, rows), rows), :] = block_ref[...]

    flip = (
        lax.broadcasted_iota(jnp.int32, (LANES, LANES), 0)
        + lax.broadcasted_iota(jnp.int32, (LANES, LANES), 1)
        == LANES - 1
    ).astype(jnp.bfloat16)
    q_all = q_ref[...].astype(jnp.float32)
    parts = []
    for p in range(per_device):
        pieces = [q_all[p : p + 1, LANES * a : LANES * (a + 1)] for a in range(q_rows)]
        parts += pieces + [jnp.zeros((q_pad - q_rows, LANES), jnp.float32)]
    q_points = jnp.concatenate(parts, axis=0)
    q_scale_ref[...] = window_stats(q_points)[1]
    q_back = jnp.dot(q_points.astype(jnp.bfloat16), flip, preferred_element_type=jnp.float32)
    for p in range(per_device):
        q_base = p * q_pad
        for a in range(full + HALVES):
            tile = toeplitz(
                q_back[q_base + a : q_base + a + 1], q_back[q_base + a + 1 : q_base + a + 2]
            ).astype(jnp.bfloat16)
            for h in range(HALVES):
                if 0 <= a - h < full:
                    left_ref[p, pl.ds((a - h) * LANES, LANES), pl.ds(h * LANES, LANES)] = tile
                elif a - h == full:
                    left_ref[p, pl.ds(full * LANES, 16), pl.ds(h * LANES, LANES)] = tile[:16]
        mean_ref[p] = jnp.dot(
            left_ref[p], jnp.full((M, LANES), 1.0 / M, jnp.bfloat16), preferred_element_type=jnp.float32
        )

    pl.semaphore_wait(barrier, members - 1)
    outgoing = to_peers(members, block_ref, series_ref, send_sem, recv_sem, False)
    incoming = to_peers(members, block_ref, series_ref, send_sem, recv_sem, True)

    @pl.loop(1, members)
    def _(d):
        outgoing(d).start()

    @pl.loop(1, members)
    def _(d):
        incoming(d).wait_recv()

    @pl.loop(1, members)
    def _(d):
        outgoing(d).wait_send()

    column = lax.broadcasted_iota(jnp.int32, (r_pad, all_rows), 1)
    wanted = lax.broadcasted_iota(jnp.int32, (r_pad, all_rows), 0)
    picks = [
        jnp.where(column == wanted + groups_ref[p] * rows, 1.0, 0.0).astype(jnp.bfloat16)
        for p in range(per_device)
    ]
    points = jnp.dot(
        jnp.concatenate(picks, axis=0), series_ref[...], preferred_element_type=jnp.float32
    )
    total, scale = window_stats(points)
    total_ref[...] = total
    scale_ref[...] = scale

    for p in range(per_device):
        r_base = p * r_pad
        q_base = p * q_pad
        for m in range(rows + 1):
            right_ref[m] = hankel(
                points[r_base + m : r_base + m + 1], points[r_base + m + 1 : r_base + m + 2]
            ).astype(jnp.bfloat16)

        g = groups_ref[p]

        def chunk(first, last):
            right = jnp.concatenate(
                [
                    jnp.concatenate([right_ref[first + h + n] for n in range(CHUNK)], axis=1)
                    for h in range(HALVES)
                ],
                axis=0,
            )
            products = jnp.dot(left_ref[p], right, preferred_element_type=jnp.float32)
            totals = [total_ref[pl.ds(r_base + first + n, 1), :] for n in range(CHUNK)]
            scales = [scale_ref[pl.ds(r_base + first + n, 1), :] for n in range(CHUNK)]
            if last:
                lane = lax.broadcasted_iota(jnp.int32, (1, LANES), 1)
                start = (g * rows + first) * LANES
                limit = all_rows * LANES - M
                floors = [
                    jnp.where(start + n * LANES + lane <= limit, 0.0, MASKED) for n in range(CHUNK)
                ]
            for t in range(0, tall, 16):
                mean = mean_ref[p, pl.ds(t, 16), :]
                best = None
                for n in range(CHUNK):
                    piece = products[t : t + 16, n * LANES : (n + 1) * LANES]
                    value = (piece - mean * totals[n]) * scales[n]
                    if last:
                        value = value + floors[n]
                    best = value if best is None else jnp.maximum(best, value)
                if not last:
                    best = jnp.maximum(best, acc_ref[pl.ds(t, 16), :])
                acc_ref[pl.ds(t, 16), :] = best

        chunk(rows - CHUNK, True)

        @pl.loop(0, rows // CHUNK - 1)
        def _(c):
            chunk(c * CHUNK, False)

        lane = lax.broadcasted_iota(jnp.int32, (1, LANES), 1)
        limit = lengths_ref[p] - M
        for a in range(q_rows):
            if a < full:
                block = acc_ref[pl.ds(a * LANES, LANES), :]
                best = jnp.max(block.T, axis=0, keepdims=True)
            elif a == full:
                block = acc_ref[pl.ds(a * LANES, 8), :]
                best = jnp.broadcast_to(jnp.max(block, axis=1, keepdims=True)[:1], (1, LANES))
            if a <= full:
                best = best * q_scale_ref[pl.ds(q_base + a, 1), :] * (1.0 / M)
                row = jnp.where(a * LANES + lane <= limit, 2.0 * (1.0 - best), 0.0)
            else:
                row = jnp.zeros((1, LANES), jnp.float32)
            out_ref[pl.ds(p, 1), pl.ds(a * LANES, LANES)] = row


def join(members, groups, lengths, queries, block):
    per_device, series_len = queries.shape
    rows = block.shape[0]
    tall = (series_len - M) // LANES * LANES + 16
    r_rows = per_device * (rows + 8)
    q_rows = per_device * (series_len // LANES + 8)
    vmem = pl.BlockSpec(memory_space=pltpu.VMEM)
    smem = pl.BlockSpec(memory_space=pltpu.SMEM)
    return pl.pallas_call(
        functools.partial(join_kernel, members),
        out_shape=jax.ShapeDtypeStruct((per_device, series_len), jnp.float32),
        in_specs=[smem, smem, vmem, vmem],
        out_specs=vmem,
        scratch_shapes=[
            pltpu.VMEM((members * rows, LANES), jnp.bfloat16),
            pltpu.VMEM((per_device, tall, M), jnp.bfloat16),
            pltpu.VMEM((rows + 1, LANES, LANES), jnp.bfloat16),
            pltpu.VMEM((per_device, tall, LANES), jnp.float32),
            pltpu.VMEM((r_rows, LANES), jnp.float32),
            pltpu.VMEM((r_rows, LANES), jnp.float32),
            pltpu.VMEM((q_rows, LANES), jnp.float32),
            pltpu.VMEM((tall, LANES), jnp.float32),
            pltpu.SemaphoreType.DMA((members,)),
            pltpu.SemaphoreType.DMA((members,)),
        ],
        compiler_params=pltpu.CompilerParams(collective_id=0, has_side_effects=True),
        name="join",
    )(groups, lengths, queries, block)


def body(long_series, queries, lengths, groups):
    members = lax.axis_size("ref")
    return join(members, groups, lengths, queries, long_series.reshape(-1, LANES))


def solution(mesh):
    in_specs = (
        P(("groups", "ref")),
        P(("groups", "ref"), None),
        P(("groups", "ref")),
        P(("groups", "ref")),
    )
    out_specs = P(("groups", "ref"), None)
    return jax.shard_map(body, mesh=mesh, in_specs=in_specs, out_specs=out_specs, check_vma=False)
```

```python
import functools

import jax
import jax.numpy as jnp
from jax import lax
from jax.experimental import pallas as pl
from jax.experimental.pallas import tpu as pltpu
from jax.sharding import PartitionSpec as P

M = 256
LANES = 128
HALVES = M // LANES
SPREAD_FLOOR = 0.25
CHUNK = 4
MASKED = -1e30
NEAR = 4


def hankel(row, following):
    shape = (LANES, LANES)
    lane = lax.broadcasted_iota(jnp.int32, shape, 1)
    sub = lax.broadcasted_iota(jnp.int32, shape, 0)
    here = pltpu.roll(jnp.broadcast_to(row, shape), 1, 1, stride=1, stride_axis=0)
    there = pltpu.roll(jnp.broadcast_to(following, shape), 1, 1, stride=1, stride_axis=0)
    return jnp.where(lane <= sub, here, there)


def toeplitz(row, following):
    shape = (LANES, LANES)
    lane = lax.broadcasted_iota(jnp.int32, shape, 1)
    sub = lax.broadcasted_iota(jnp.int32, shape, 0)
    here = pltpu.roll(jnp.broadcast_to(row, shape), 0, 1, stride=1, stride_axis=0)
    there = pltpu.roll(jnp.broadcast_to(following, shape), 0, 1, stride=1, stride_axis=0)
    return jnp.where(lane >= sub, here, there)


def next_row(x):
    return pltpu.roll(x, x.shape[0] - 1, 0)


def window_stats(x):
    lane = lax.broadcasted_iota(jnp.int32, x.shape, 1)
    total, square = x, jnp.zeros_like(x)
    count = 1
    while count < M:
        def ahead(v):
            if count == LANES:
                return next_row(v)
            rolled = pltpu.roll(v, LANES - count, 1)
            return jnp.where(lane < LANES - count, rolled, next_row(rolled))

        total_ahead, square_ahead = ahead(total), ahead(square)
        gap = total - total_ahead
        square = square + square_ahead + gap * gap * (0.5 / count)
        total = total + total_ahead
        count *= 2
    return total, 1.0 / jnp.sqrt(square * (1.0 / M) + SPREAD_FLOOR)


def ring_order(count):
    return sorted(range(1, count), key=lambda d: (min(d, count - d), d))


def join_kernel(members, groups_hbm, lengths_hbm, q_hbm, block_hbm, out_ref,
                series_ref, left_ref, right_ref, mean_ref, total_ref, scale_ref, q_scale_ref, acc_ref,
                q_ref, groups_ref, lengths_ref,
                local_sem, far_send, far_recv, near_send, near_recv):
    per_device, series_len = q_ref.shape
    q_rows = series_len // LANES
    all_rows = series_ref.shape[0]
    rows = all_rows // members
    full = (series_len - M) // LANES
    tall = full * LANES + 16
    r_pad = rows + 8
    q_pad = q_rows + 8
    near = NEAR if members % NEAR == 0 else 1
    far = members // near
    me = lax.axis_index("ref")
    high, low = me // near, lax.rem(me, near)

    def far_place(d):
        return lax.rem(high + d, far) * near + low

    def near_place(e):
        return high * near + lax.rem(low + e, near)

    def slot(owner):
        return series_ref.at[pl.ds(pl.multiple_of(owner * rows, rows), rows), :]

    def far_copy(d, owner):
        return pltpu.make_async_remote_copy(
            src_ref=slot(me), dst_ref=slot(owner), send_sem=far_send.at[d], recv_sem=far_recv.at[d],
            device_id={"ref": far_place(d)}, device_id_type=pl.DeviceIdType.MESH,
        )

    def near_copy(e, d, owner):
        return pltpu.make_async_remote_copy(
            src_ref=slot(owner), dst_ref=slot(owner),
            send_sem=near_send.at[e * far + d], recv_sem=near_recv.at[e * far + d],
            device_id={"ref": near_place(e)}, device_id_type=pl.DeviceIdType.MESH,
        )

    fetches = [
        pltpu.make_async_copy(block_hbm, slot(me), local_sem.at[0]),
        pltpu.make_async_copy(q_hbm, q_ref, local_sem.at[1]),
        pltpu.make_async_copy(groups_hbm, groups_ref, local_sem.at[2]),
        pltpu.make_async_copy(lengths_hbm, lengths_ref, local_sem.at[3]),
    ]
    barrier = pltpu.get_barrier_semaphore()
    peers = [far_place(d) for d in reversed(ring_order(far))] + [near_place(e) for e in range(1, near)]
    for peer in peers:
        pl.semaphore_signal(
            barrier, inc=1, device_id={"ref": peer}, device_id_type=pl.DeviceIdType.MESH
        )
    for fetch in fetches:
        fetch.start()
    fetches[1].wait()

    flip = (
        lax.broadcasted_iota(jnp.int32, (LANES, LANES), 0)
        + lax.broadcasted_iota(jnp.int32, (LANES, LANES), 1)
        == LANES - 1
    ).astype(jnp.bfloat16)
    q_all = q_ref[...].astype(jnp.float32)
    parts = []
    for p in range(per_device):
        pieces = [q_all[p : p + 1, LANES * a : LANES * (a + 1)] for a in range(q_rows)]
        parts += pieces + [jnp.zeros((q_pad - q_rows, LANES), jnp.float32)]
    q_points = jnp.concatenate(parts, axis=0)
    q_scale_ref[...] = window_stats(q_points)[1]
    q_back = jnp.dot(q_points.astype(jnp.bfloat16), flip, preferred_element_type=jnp.float32)
    for p in range(per_device):
        q_base = p * q_pad
        for a in range(full + HALVES):
            tile = toeplitz(
                q_back[q_base + a : q_base + a + 1], q_back[q_base + a + 1 : q_base + a + 2]
            ).astype(jnp.bfloat16)
            for h in range(HALVES):
                if 0 <= a - h < full:
                    left_ref[p, pl.ds((a - h) * LANES, LANES), pl.ds(h * LANES, LANES)] = tile
                elif a - h == full:
                    left_ref[p, pl.ds(full * LANES, 16), pl.ds(h * LANES, LANES)] = tile[:16]
        mean_ref[p] = jnp.dot(
            left_ref[p], jnp.full((M, LANES), 1.0 / M, jnp.bfloat16), preferred_element_type=jnp.float32
        )

    fetches[0].wait()
    pl.semaphore_wait(barrier, len(peers))
    for d in reversed(ring_order(far)):
        far_copy(d, me).start()
    for e in range(1, near):
        near_copy(e, 0, me).start()
    for d in ring_order(far):
        owner = far_place(far - d)
        far_copy(d, owner).wait_recv()
        for e in range(1, near):
            near_copy(e, d, owner).start()
    fetches[2].wait()
    fetches[3].wait()
    for d in [0] + ring_order(far):
        for e in range(1, near):
            owner = lax.rem(high + far - d, far) * near + lax.rem(low + near - e, near)
            near_copy(e, d, owner).wait_recv()

    column = lax.broadcasted_iota(jnp.int32, (r_pad, all_rows), 1)
    wanted = lax.broadcasted_iota(jnp.int32, (r_pad, all_rows), 0)
    picks = [
        jnp.where(column == wanted + groups_ref[p] * rows, 1.0, 0.0).astype(jnp.bfloat16)
        for p in range(per_device)
    ]
    points = jnp.dot(
        jnp.concatenate(picks, axis=0), series_ref[...], preferred_element_type=jnp.float32
    )
    total, scale = window_stats(points)
    total_ref[...] = total
    scale_ref[...] = scale

    for p in range(per_device):
        r_base = p * r_pad
        q_base = p * q_pad
        for m in range(rows + 1):
            right_ref[m] = hankel(
                points[r_base + m : r_base + m + 1], points[r_base + m + 1 : r_base + m + 2]
            ).astype(jnp.bfloat16)

        g = groups_ref[p]

        def chunk(first, last):
            right = jnp.concatenate(
                [
                    jnp.concatenate([right_ref[first + h + n] for n in range(CHUNK)], axis=1)
                    for h in range(HALVES)
                ],
                axis=0,
            )
            products = jnp.dot(left_ref[p], right, preferred_element_type=jnp.float32)
            totals = [total_ref[pl.ds(r_base + first + n, 1), :] for n in range(CHUNK)]
            scales = [scale_ref[pl.ds(r_base + first + n, 1), :] for n in range(CHUNK)]
            if last:
                lane = lax.broadcasted_iota(jnp.int32, (1, LANES), 1)
                start = (g * rows + first) * LANES
                limit = all_rows * LANES - M
                floors = [
                    jnp.where(start + n * LANES + lane <= limit, 0.0, MASKED) for n in range(CHUNK)
                ]
            for t in range(0, tall, 16):
                mean = mean_ref[p, pl.ds(t, 16), :]
                best = None
                for n in range(CHUNK):
                    piece = products[t : t + 16, n * LANES : (n + 1) * LANES]
                    value = (piece - mean * totals[n]) * scales[n]
                    if last:
                        value = value + floors[n]
                    best = value if best is None else jnp.maximum(best, value)
                if not last:
                    best = jnp.maximum(best, acc_ref[pl.ds(t, 16), :])
                acc_ref[pl.ds(t, 16), :] = best

        chunk(rows - CHUNK, True)

        @pl.loop(0, rows // CHUNK - 1)
        def _(c):
            chunk(c * CHUNK, False)

        lane = lax.broadcasted_iota(jnp.int32, (1, LANES), 1)
        limit = lengths_ref[p] - M
        for a in range(q_rows):
            if a < full:
                block = acc_ref[pl.ds(a * LANES, LANES), :]
                best = jnp.max(block.T, axis=0, keepdims=True)
            elif a == full:
                block = acc_ref[pl.ds(a * LANES, 8), :]
                best = jnp.broadcast_to(jnp.max(block, axis=1, keepdims=True)[:1], (1, LANES))
            if a <= full:
                best = best * q_scale_ref[pl.ds(q_base + a, 1), :] * (1.0 / M)
                row = jnp.where(a * LANES + lane <= limit, 2.0 * (1.0 - best), 0.0)
            else:
                row = jnp.zeros((1, LANES), jnp.float32)
            out_ref[pl.ds(p, 1), pl.ds(a * LANES, LANES)] = row

    for d in ring_order(far):
        far_copy(d, me).wait_send()
    for d in range(far):
        for e in range(1, near):
            near_copy(e, d, far_place(far - d)).wait_send()


def join(members, groups, lengths, queries, block):
    per_device, series_len = queries.shape
    rows = block.shape[0]
    tall = (series_len - M) // LANES * LANES + 16
    r_rows = per_device * (rows + 8)
    q_rows = per_device * (series_len // LANES + 8)
    vmem = pl.BlockSpec(memory_space=pltpu.VMEM)
    return pl.pallas_call(
        functools.partial(join_kernel, members),
        out_shape=jax.ShapeDtypeStruct((per_device, series_len), jnp.float32),
        in_specs=[pl.BlockSpec(memory_space=pl.ANY)] * 4,
        out_specs=vmem,
        scratch_shapes=[
            pltpu.VMEM((members * rows, LANES), jnp.bfloat16),
            pltpu.VMEM((per_device, tall, M), jnp.bfloat16),
            pltpu.VMEM((rows + 1, LANES, LANES), jnp.bfloat16),
            pltpu.VMEM((per_device, tall, LANES), jnp.float32),
            pltpu.VMEM((r_rows, LANES), jnp.float32),
            pltpu.VMEM((r_rows, LANES), jnp.float32),
            pltpu.VMEM((q_rows, LANES), jnp.float32),
            pltpu.VMEM((tall, LANES), jnp.float32),
            pltpu.VMEM((per_device, series_len), jnp.bfloat16),
            pltpu.SMEM((per_device,), jnp.int32),
            pltpu.SMEM((per_device,), jnp.int32),
            pltpu.SemaphoreType.DMA((4,)),
            pltpu.SemaphoreType.DMA((members,)),
            pltpu.SemaphoreType.DMA((members,)),
            pltpu.SemaphoreType.DMA((NEAR * members,)),
            pltpu.SemaphoreType.DMA((NEAR * members,)),
        ],
        compiler_params=pltpu.CompilerParams(collective_id=0, has_side_effects=True),
        name="join",
    )(groups, lengths, queries, block)


def body(long_series, queries, lengths, groups):
    members = lax.axis_size("ref")
    return join(members, groups, lengths, queries, long_series.reshape(-1, LANES))


def solution(mesh):
    in_specs = (
        P(("groups", "ref")),
        P(("groups", "ref"), None),
        P(("groups", "ref")),
        P(("groups", "ref")),
    )
    out_specs = P(("groups", "ref"), None)
    return jax.shard_map(body, mesh=mesh, in_specs=in_specs, out_specs=out_specs, check_vma=False)
```

```python
import functools

import jax
import jax.numpy as jnp
from jax import lax
from jax.experimental import pallas as pl
from jax.experimental.pallas import tpu as pltpu
from jax.sharding import PartitionSpec as P

M = 256
LANES = 128
HALVES = M // LANES
SPREAD_FLOOR = 0.25
CHUNK = 4
MASKED = -1e30
NEAR = 1


def hankel(row, following):
    shape = (LANES, LANES)
    lane = lax.broadcasted_iota(jnp.int32, shape, 1)
    sub = lax.broadcasted_iota(jnp.int32, shape, 0)
    here = pltpu.roll(jnp.broadcast_to(row, shape), 1, 1, stride=1, stride_axis=0)
    there = pltpu.roll(jnp.broadcast_to(following, shape), 1, 1, stride=1, stride_axis=0)
    return jnp.where(lane <= sub, here, there)


def toeplitz(row, following):
    shape = (LANES, LANES)
    lane = lax.broadcasted_iota(jnp.int32, shape, 1)
    sub = lax.broadcasted_iota(jnp.int32, shape, 0)
    here = pltpu.roll(jnp.broadcast_to(row, shape), 0, 1, stride=1, stride_axis=0)
    there = pltpu.roll(jnp.broadcast_to(following, shape), 0, 1, stride=1, stride_axis=0)
    return jnp.where(lane >= sub, here, there)


def next_row(x):
    return pltpu.roll(x, x.shape[0] - 1, 0)


def window_stats(x):
    lane = lax.broadcasted_iota(jnp.int32, x.shape, 1)
    total, square = x, jnp.zeros_like(x)
    count = 1
    while count < M:
        def ahead(v):
            if count == LANES:
                return next_row(v)
            rolled = pltpu.roll(v, LANES - count, 1)
            return jnp.where(lane < LANES - count, rolled, next_row(rolled))

        total_ahead, square_ahead = ahead(total), ahead(square)
        gap = total - total_ahead
        square = square + square_ahead + gap * gap * (0.5 / count)
        total = total + total_ahead
        count *= 2
    return total, 1.0 / jnp.sqrt(square * (1.0 / M) + SPREAD_FLOOR)


def ring_order(count):
    return sorted(range(1, count), key=lambda d: (min(d, count - d), d))


def join_kernel(members, groups_hbm, lengths_hbm, q_hbm, block_hbm, out_ref,
                series_ref, left_ref, right_ref, mean_ref, total_ref, scale_ref, q_scale_ref, acc_ref,
                q_ref, groups_ref, lengths_ref,
                local_sem, far_send, far_recv, near_send, near_recv):
    per_device, series_len = q_ref.shape
    q_rows = series_len // LANES
    all_rows = series_ref.shape[0]
    rows = all_rows // members
    full = (series_len - M) // LANES
    tall = full * LANES + 16
    r_pad = rows + 8
    q_pad = q_rows + 8
    near = NEAR if members % NEAR == 0 else 1
    far = members // near
    me = lax.axis_index("ref")
    high, low = me // near, lax.rem(me, near)

    def far_place(d):
        return lax.rem(high + d, far) * near + low

    def near_place(e):
        return high * near + lax.rem(low + e, near)

    def slot(owner):
        return series_ref.at[pl.ds(pl.multiple_of(owner * rows, rows), rows), :]

    def far_copy(d, owner):
        return pltpu.make_async_remote_copy(
            src_ref=slot(me), dst_ref=slot(owner), send_sem=far_send.at[d], recv_sem=far_recv.at[d],
            device_id={"ref": far_place(d)}, device_id_type=pl.DeviceIdType.MESH,
        )

    def near_copy(e, d, owner):
        return pltpu.make_async_remote_copy(
            src_ref=slot(owner), dst_ref=slot(owner),
            send_sem=near_send.at[e * far + d], recv_sem=near_recv.at[e * far + d],
            device_id={"ref": near_place(e)}, device_id_type=pl.DeviceIdType.MESH,
        )

    fetches = [
        pltpu.make_async_copy(block_hbm, slot(me), local_sem.at[0]),
        pltpu.make_async_copy(q_hbm, q_ref, local_sem.at[1]),
        pltpu.make_async_copy(groups_hbm, groups_ref, local_sem.at[2]),
        pltpu.make_async_copy(lengths_hbm, lengths_ref, local_sem.at[3]),
    ]
    barrier = pltpu.get_barrier_semaphore()
    peers = [far_place(d) for d in reversed(ring_order(far))] + [near_place(e) for e in range(1, near)]
    for peer in peers:
        pl.semaphore_signal(
            barrier, inc=1, device_id={"ref": peer}, device_id_type=pl.DeviceIdType.MESH
        )
    for fetch in fetches:
        fetch.start()
    fetches[1].wait()

    flip = (
        lax.broadcasted_iota(jnp.int32, (LANES, LANES), 0)
        + lax.broadcasted_iota(jnp.int32, (LANES, LANES), 1)
        == LANES - 1
    ).astype(jnp.bfloat16)
    q_all = q_ref[...].astype(jnp.float32)
    parts = []
    for p in range(per_device):
        pieces = [q_all[p : p + 1, LANES * a : LANES * (a + 1)] for a in range(q_rows)]
        parts += pieces + [jnp.zeros((q_pad - q_rows, LANES), jnp.float32)]
    q_points = jnp.concatenate(parts, axis=0)
    q_scale_ref[...] = window_stats(q_points)[1]
    q_back = jnp.dot(q_points.astype(jnp.bfloat16), flip, preferred_element_type=jnp.float32)
    for p in range(per_device):
        q_base = p * q_pad
        for a in range(full + HALVES):
            tile = toeplitz(
                q_back[q_base + a : q_base + a + 1], q_back[q_base + a + 1 : q_base + a + 2]
            ).astype(jnp.bfloat16)
            for h in range(HALVES):
                if 0 <= a - h < full:
                    left_ref[p, pl.ds((a - h) * LANES, LANES), pl.ds(h * LANES, LANES)] = tile
                elif a - h == full:
                    left_ref[p, pl.ds(full * LANES, 16), pl.ds(h * LANES, LANES)] = tile[:16]
        mean_ref[p] = jnp.dot(
            left_ref[p], jnp.full((M, LANES), 1.0 / M, jnp.bfloat16), preferred_element_type=jnp.float32
        )

    fetches[0].wait()
    pl.semaphore_wait(barrier, len(peers))
    for d in reversed(ring_order(far)):
        far_copy(d, me).start()
    for e in range(1, near):
        near_copy(e, 0, me).start()
    for d in ring_order(far):
        owner = far_place(far - d)
        far_copy(d, owner).wait_recv()
        for e in range(1, near):
            near_copy(e, d, owner).start()
    fetches[2].wait()
    fetches[3].wait()
    for d in [0] + ring_order(far):
        for e in range(1, near):
            owner = lax.rem(high + far - d, far) * near + lax.rem(low + near - e, near)
            near_copy(e, d, owner).wait_recv()

    column = lax.broadcasted_iota(jnp.int32, (r_pad, all_rows), 1)
    wanted = lax.broadcasted_iota(jnp.int32, (r_pad, all_rows), 0)
    picks = [
        jnp.where(column == wanted + groups_ref[p] * rows, 1.0, 0.0).astype(jnp.bfloat16)
        for p in range(per_device)
    ]
    points = jnp.dot(
        jnp.concatenate(picks, axis=0), series_ref[...], preferred_element_type=jnp.float32
    )
    total, scale = window_stats(points)
    total_ref[...] = total
    scale_ref[...] = scale

    for p in range(per_device):
        r_base = p * r_pad
        q_base = p * q_pad
        for m in range(rows + 1):
            right_ref[m] = hankel(
                points[r_base + m : r_base + m + 1], points[r_base + m + 1 : r_base + m + 2]
            ).astype(jnp.bfloat16)

        g = groups_ref[p]

        def chunk(first, last):
            right = jnp.concatenate(
                [
                    jnp.concatenate([right_ref[first + h + n] for n in range(CHUNK)], axis=1)
                    for h in range(HALVES)
                ],
                axis=0,
            )
            products = jnp.dot(left_ref[p], right, preferred_element_type=jnp.float32)
            totals = [total_ref[pl.ds(r_base + first + n, 1), :] for n in range(CHUNK)]
            scales = [scale_ref[pl.ds(r_base + first + n, 1), :] for n in range(CHUNK)]
            if last:
                lane = lax.broadcasted_iota(jnp.int32, (1, LANES), 1)
                start = (g * rows + first) * LANES
                limit = all_rows * LANES - M
                floors = [
                    jnp.where(start + n * LANES + lane <= limit, 0.0, MASKED) for n in range(CHUNK)
                ]
            for t in range(0, tall, 16):
                mean = mean_ref[p, pl.ds(t, 16), :]
                best = None
                for n in range(CHUNK):
                    piece = products[t : t + 16, n * LANES : (n + 1) * LANES]
                    value = (piece - mean * totals[n]) * scales[n]
                    if last:
                        value = value + floors[n]
                    best = value if best is None else jnp.maximum(best, value)
                if not last:
                    best = jnp.maximum(best, acc_ref[pl.ds(t, 16), :])
                acc_ref[pl.ds(t, 16), :] = best

        chunk(rows - CHUNK, True)

        @pl.loop(0, rows // CHUNK - 1)
        def _(c):
            chunk(c * CHUNK, False)

        lane = lax.broadcasted_iota(jnp.int32, (1, LANES), 1)
        limit = lengths_ref[p] - M
        for a in range(q_rows):
            if a < full:
                block = acc_ref[pl.ds(a * LANES, LANES), :]
                best = jnp.max(block.T, axis=0, keepdims=True)
            elif a == full:
                block = acc_ref[pl.ds(a * LANES, 8), :]
                best = jnp.broadcast_to(jnp.max(block, axis=1, keepdims=True)[:1], (1, LANES))
            if a <= full:
                best = best * q_scale_ref[pl.ds(q_base + a, 1), :] * (1.0 / M)
                row = jnp.where(a * LANES + lane <= limit, 2.0 * (1.0 - best), 0.0)
            else:
                row = jnp.zeros((1, LANES), jnp.float32)
            out_ref[pl.ds(p, 1), pl.ds(a * LANES, LANES)] = row

    for d in ring_order(far):
        far_copy(d, me).wait_send()
    for d in range(far):
        for e in range(1, near):
            near_copy(e, d, far_place(far - d)).wait_send()


def join(members, groups, lengths, queries, block):
    per_device, series_len = queries.shape
    rows = block.shape[0]
    tall = (series_len - M) // LANES * LANES + 16
    r_rows = per_device * (rows + 8)
    q_rows = per_device * (series_len // LANES + 8)
    vmem = pl.BlockSpec(memory_space=pltpu.VMEM)
    return pl.pallas_call(
        functools.partial(join_kernel, members),
        out_shape=jax.ShapeDtypeStruct((per_device, series_len), jnp.float32),
        in_specs=[pl.BlockSpec(memory_space=pl.ANY)] * 4,
        out_specs=vmem,
        scratch_shapes=[
            pltpu.VMEM((members * rows, LANES), jnp.bfloat16),
            pltpu.VMEM((per_device, tall, M), jnp.bfloat16),
            pltpu.VMEM((rows + 1, LANES, LANES), jnp.bfloat16),
            pltpu.VMEM((per_device, tall, LANES), jnp.float32),
            pltpu.VMEM((r_rows, LANES), jnp.float32),
            pltpu.VMEM((r_rows, LANES), jnp.float32),
            pltpu.VMEM((q_rows, LANES), jnp.float32),
            pltpu.VMEM((tall, LANES), jnp.float32),
            pltpu.VMEM((per_device, series_len), jnp.bfloat16),
            pltpu.SMEM((per_device,), jnp.int32),
            pltpu.SMEM((per_device,), jnp.int32),
            pltpu.SemaphoreType.DMA((4,)),
            pltpu.SemaphoreType.DMA((members,)),
            pltpu.SemaphoreType.DMA((members,)),
            pltpu.SemaphoreType.DMA((NEAR * members,)),
            pltpu.SemaphoreType.DMA((NEAR * members,)),
        ],
        compiler_params=pltpu.CompilerParams(collective_id=0, has_side_effects=True),
        name="join",
    )(groups, lengths, queries, block)


def body(long_series, queries, lengths, groups):
    members = lax.axis_size("ref")
    return join(members, groups, lengths, queries, long_series.reshape(-1, LANES))


def solution(mesh):
    in_specs = (
        P(("groups", "ref")),
        P(("groups", "ref"), None),
        P(("groups", "ref")),
        P(("groups", "ref")),
    )
    out_specs = P(("groups", "ref"), None)
    return jax.shard_map(body, mesh=mesh, in_specs=in_specs, out_specs=out_specs, check_vma=False)
```

```python
import functools

import jax
import jax.numpy as jnp
from jax import lax
from jax.experimental import pallas as pl
from jax.experimental.pallas import tpu as pltpu
from jax.sharding import PartitionSpec as P

M = 256
LANES = 128
HALVES = M // LANES
SPREAD_FLOOR = 0.25
CHUNK = 4
MASKED = -1e30


def hankel_tiles(rows):
    shape = (LANES, LANES)
    lane = lax.broadcasted_iota(jnp.int32, shape, 1)
    sub = lax.broadcasted_iota(jnp.int32, shape, 0)
    rolled = [
        pltpu.roll(jnp.broadcast_to(row, shape), 1, 1, stride=1, stride_axis=0) for row in rows
    ]
    return [
        jnp.where(lane <= sub, here, there).astype(jnp.bfloat16)
        for here, there in zip(rolled, rolled[1:])
    ]


def toeplitz(row, following):
    shape = (LANES, LANES)
    lane = lax.broadcasted_iota(jnp.int32, shape, 1)
    sub = lax.broadcasted_iota(jnp.int32, shape, 0)
    here = pltpu.roll(jnp.broadcast_to(row, shape), 0, 1, stride=1, stride_axis=0)
    there = pltpu.roll(jnp.broadcast_to(following, shape), 0, 1, stride=1, stride_axis=0)
    return jnp.where(lane >= sub, here, there)


def next_row(x):
    return pltpu.roll(x, x.shape[0] - 1, 0)


def window_stats(x):
    lane = lax.broadcasted_iota(jnp.int32, x.shape, 1)
    total, square = x, jnp.zeros_like(x)
    count = 1
    while count < M:
        def ahead(v):
            if count == LANES:
                return next_row(v)
            rolled = pltpu.roll(v, LANES - count, 1)
            return jnp.where(lane < LANES - count, rolled, next_row(rolled))

        total_ahead, square_ahead = ahead(total), ahead(square)
        gap = total - total_ahead
        square = square + square_ahead + gap * gap * (0.5 / count)
        total = total + total_ahead
        count *= 2
    return total, 1.0 / jnp.sqrt(square * (1.0 / M) + SPREAD_FLOOR)


def join_kernel(members, groups_hbm, lengths_hbm, q_hbm, block_hbm, out_ref,
                series_ref, left_ref, right_ref, mean_ref, total_ref, scale_ref, q_scale_ref, acc_ref,
                q_ref, groups_ref, lengths_ref,
                local_sem, send_sem, recv_sem):
    per_device, series_len = q_ref.shape
    q_rows = series_len // LANES
    all_rows = series_ref.shape[0]
    rows = all_rows // members
    full = (series_len - M) // LANES
    tall = full * LANES + 16
    r_pad = rows + 16
    q_pad = q_rows + 8
    me = lax.axis_index("ref")

    def place(d):
        return lax.rem(me + d, members)

    def slot(owner):
        return series_ref.at[pl.ds(pl.multiple_of(owner * rows, rows), rows), :]

    def copy(d, owner):
        return pltpu.make_async_remote_copy(
            src_ref=slot(me), dst_ref=slot(owner), send_sem=send_sem.at[d], recv_sem=recv_sem.at[d],
            device_id={"ref": place(d)}, device_id_type=pl.DeviceIdType.MESH,
        )

    fetches = [
        pltpu.make_async_copy(block_hbm, slot(me), local_sem.at[0]),
        pltpu.make_async_copy(q_hbm, q_ref, local_sem.at[1]),
        pltpu.make_async_copy(groups_hbm, groups_ref, local_sem.at[2]),
        pltpu.make_async_copy(lengths_hbm, lengths_ref, local_sem.at[3]),
    ]
    barrier = pltpu.get_barrier_semaphore()
    for fetch in fetches:
        fetch.start()

    @pl.loop(1, members)
    def _(d):
        pl.semaphore_signal(
            barrier, inc=1, device_id={"ref": place(d)}, device_id_type=pl.DeviceIdType.MESH
        )

    fetches[1].wait()

    flip = (
        lax.broadcasted_iota(jnp.int32, (LANES, LANES), 0)
        + lax.broadcasted_iota(jnp.int32, (LANES, LANES), 1)
        == LANES - 1
    ).astype(jnp.bfloat16)
    q_all = q_ref[...].astype(jnp.float32)
    parts = []
    for p in range(per_device):
        pieces = [q_all[p : p + 1, LANES * a : LANES * (a + 1)] for a in range(q_rows)]
        parts += pieces + [jnp.zeros((q_pad - q_rows, LANES), jnp.float32)]
    q_points = jnp.concatenate(parts, axis=0)
    q_scale_ref[...] = window_stats(q_points)[1]
    q_back = jnp.dot(q_points.astype(jnp.bfloat16), flip, preferred_element_type=jnp.float32)
    for p in range(per_device):
        q_base = p * q_pad
        for a in range(full + HALVES):
            tile = toeplitz(
                q_back[q_base + a : q_base + a + 1], q_back[q_base + a + 1 : q_base + a + 2]
            ).astype(jnp.bfloat16)
            for h in range(HALVES):
                if 0 <= a - h < full:
                    left_ref[p, pl.ds((a - h) * LANES, LANES), pl.ds(h * LANES, LANES)] = tile
                elif a - h == full:
                    left_ref[p, pl.ds(full * LANES, 16), pl.ds(h * LANES, LANES)] = tile[:16]
        mean_ref[p] = jnp.dot(
            left_ref[p], jnp.full((M, LANES), 1.0 / M, jnp.bfloat16), preferred_element_type=jnp.float32
        )

    fetches[0].wait()
    pl.semaphore_wait(barrier, members - 1)

    @pl.loop(1, members)
    def _(d):
        copy(d, me).start()

    fetches[2].wait()
    fetches[3].wait()

    @pl.loop(1, members)
    def _(d):
        copy(d, place(members - d)).wait_recv()

    column = lax.broadcasted_iota(jnp.int32, (r_pad, all_rows), 1)
    wanted = lax.broadcasted_iota(jnp.int32, (r_pad, all_rows), 0)
    picks = [
        jnp.where(column == wanted + groups_ref[p] * rows, 1.0, 0.0).astype(jnp.bfloat16)
        for p in range(per_device)
    ]
    points = jnp.dot(
        jnp.concatenate(picks, axis=0), series_ref[...], preferred_element_type=jnp.float32
    )
    total, scale = window_stats(points)
    total_ref[...] = total
    scale_ref[...] = scale

    for p in range(per_device):
        r_base = p * r_pad
        q_base = p * q_pad
        tiles = hankel_tiles([points[r_base + m : r_base + m + 1] for m in range(rows + HALVES)])
        for m, tile in enumerate(tiles):
            right_ref[m] = tile

        g = groups_ref[p]

        def chunk(first, last):
            right = jnp.concatenate(
                [
                    jnp.concatenate([right_ref[first + h + n] for n in range(CHUNK)], axis=1)
                    for h in range(HALVES)
                ],
                axis=0,
            )
            products = jnp.dot(left_ref[p], right, preferred_element_type=jnp.float32)
            totals = [total_ref[pl.ds(r_base + first + n, 1), :] for n in range(CHUNK)]
            scales = [scale_ref[pl.ds(r_base + first + n, 1), :] for n in range(CHUNK)]
            if last:
                lane = lax.broadcasted_iota(jnp.int32, (1, LANES), 1)
                start = (g * rows + first) * LANES
                limit = all_rows * LANES - M
                floors = [
                    jnp.where(start + n * LANES + lane <= limit, 0.0, MASKED) for n in range(CHUNK)
                ]
            for t in range(0, tall, 16):
                mean = mean_ref[p, pl.ds(t, 16), :]
                best = None
                for n in range(CHUNK):
                    piece = products[t : t + 16, n * LANES : (n + 1) * LANES]
                    value = (piece - mean * totals[n]) * scales[n]
                    if last:
                        value = value + floors[n]
                    best = value if best is None else jnp.maximum(best, value)
                if not last:
                    best = jnp.maximum(best, acc_ref[pl.ds(t, 16), :])
                acc_ref[pl.ds(t, 16), :] = best

        chunk(rows - CHUNK, True)

        @pl.loop(0, rows // CHUNK - 1)
        def _(c):
            chunk(c * CHUNK, False)

        lane = lax.broadcasted_iota(jnp.int32, (1, LANES), 1)
        limit = lengths_ref[p] - M
        for a in range(q_rows):
            if a < full:
                block = acc_ref[pl.ds(a * LANES, LANES), :]
                best = jnp.max(block.T, axis=0, keepdims=True)
            elif a == full:
                block = acc_ref[pl.ds(a * LANES, 8), :]
                best = jnp.broadcast_to(jnp.max(block, axis=1, keepdims=True)[:1], (1, LANES))
            if a <= full:
                best = best * q_scale_ref[pl.ds(q_base + a, 1), :] * (1.0 / M)
                row = jnp.where(a * LANES + lane <= limit, 2.0 * (1.0 - best), 0.0)
            else:
                row = jnp.zeros((1, LANES), jnp.float32)
            out_ref[pl.ds(p, 1), pl.ds(a * LANES, LANES)] = row

    @pl.loop(1, members)
    def _(d):
        copy(d, me).wait_send()


def join(members, groups, lengths, queries, block):
    per_device, series_len = queries.shape
    rows = block.shape[0]
    tall = (series_len - M) // LANES * LANES + 16
    r_rows = per_device * (rows + 16)
    q_rows = per_device * (series_len // LANES + 8)
    vmem = pl.BlockSpec(memory_space=pltpu.VMEM)
    return pl.pallas_call(
        functools.partial(join_kernel, members),
        out_shape=pltpu.VMEM((per_device, series_len), jnp.float32),
        in_specs=[pl.BlockSpec(memory_space=pl.ANY)] * 4,
        out_specs=vmem,
        scratch_shapes=[
            pltpu.VMEM((members * rows, LANES), jnp.bfloat16),
            pltpu.VMEM((per_device, tall, M), jnp.bfloat16),
            pltpu.VMEM((rows + 1, LANES, LANES), jnp.bfloat16),
            pltpu.VMEM((per_device, tall, LANES), jnp.float32),
            pltpu.VMEM((r_rows, LANES), jnp.float32),
            pltpu.VMEM((r_rows, LANES), jnp.float32),
            pltpu.VMEM((q_rows, LANES), jnp.float32),
            pltpu.VMEM((tall, LANES), jnp.float32),
            pltpu.VMEM((per_device, series_len), jnp.bfloat16),
            pltpu.SMEM((per_device,), jnp.int32),
            pltpu.SMEM((per_device,), jnp.int32),
            pltpu.SemaphoreType.DMA((4,)),
            pltpu.SemaphoreType.DMA((members,)),
            pltpu.SemaphoreType.DMA((members,)),
        ],
        compiler_params=pltpu.CompilerParams(collective_id=0, has_side_effects=True),
        name="join",
    )(groups, lengths, queries, block)


def body(long_series, queries, lengths, groups):
    members = lax.axis_size("ref")
    return join(members, groups, lengths, queries, long_series.reshape(-1, LANES))


def solution(mesh):
    in_specs = (
        P(("groups", "ref")),
        P(("groups", "ref"), None),
        P(("groups", "ref")),
        P(("groups", "ref")),
    )
    out_specs = P(("groups", "ref"), None)
    return jax.shard_map(body, mesh=mesh, in_specs=in_specs, out_specs=out_specs, check_vma=False)
```

```python
import functools

import jax
import jax.numpy as jnp
from jax import lax
from jax.experimental import pallas as pl
from jax.experimental.pallas import tpu as pltpu
from jax.sharding import PartitionSpec as P

M = 256
LANES = 128
HALVES = M // LANES
SPREAD_FLOOR = 0.25
CHUNK = 4
MASKED = -1e30


def hankel_tiles(rows):
    shape = (LANES, LANES)
    lane = lax.broadcasted_iota(jnp.int32, shape, 1)
    sub = lax.broadcasted_iota(jnp.int32, shape, 0)
    rolled = [
        pltpu.roll(jnp.broadcast_to(row, shape), 1, 1, stride=1, stride_axis=0) for row in rows
    ]
    return [
        jnp.where(lane <= sub, here, there).astype(jnp.bfloat16)
        for here, there in zip(rolled, rolled[1:])
    ]


def toeplitz(row, following):
    shape = (LANES, LANES)
    lane = lax.broadcasted_iota(jnp.int32, shape, 1)
    sub = lax.broadcasted_iota(jnp.int32, shape, 0)
    here = pltpu.roll(jnp.broadcast_to(row, shape), 0, 1, stride=1, stride_axis=0)
    there = pltpu.roll(jnp.broadcast_to(following, shape), 0, 1, stride=1, stride_axis=0)
    return jnp.where(lane >= sub, here, there)


def next_row(x):
    return pltpu.roll(x, x.shape[0] - 1, 0)


def window_stats(x):
    lane = lax.broadcasted_iota(jnp.int32, x.shape, 1)
    total, square = x, jnp.zeros_like(x)
    count = 1
    while count < M:
        def ahead(v):
            if count == LANES:
                return next_row(v)
            rolled = pltpu.roll(v, LANES - count, 1)
            return jnp.where(lane < LANES - count, rolled, next_row(rolled))

        total_ahead, square_ahead = ahead(total), ahead(square)
        gap = total - total_ahead
        square = square + square_ahead + gap * gap * (0.5 / count)
        total = total + total_ahead
        count *= 2
    return total, 1.0 / jnp.sqrt(square * (1.0 / M) + SPREAD_FLOOR)


def join_kernel(members, groups_hbm, lengths_hbm, q_hbm, block_hbm, out_ref,
                series_ref, left_ref, right_ref, mean_ref, total_ref, scale_ref, q_scale_ref, acc_ref, even_ref, odd_ref,
                q_ref, groups_ref, lengths_ref,
                local_sem, send_sem, recv_sem):
    per_device, series_len = q_ref.shape
    q_rows = series_len // LANES
    all_rows = series_ref.shape[0]
    rows = all_rows // members
    full = (series_len - M) // LANES
    tall = full * LANES + 16
    r_pad = rows + 16
    q_pad = q_rows + 8
    me = lax.axis_index("ref")

    def place(d):
        return lax.rem(me + d, members)

    def slot(owner):
        return series_ref.at[pl.ds(pl.multiple_of(owner * rows, rows), rows), :]

    def copy(d, owner):
        return pltpu.make_async_remote_copy(
            src_ref=slot(me), dst_ref=slot(owner), send_sem=send_sem.at[d], recv_sem=recv_sem.at[d],
            device_id={"ref": place(d)}, device_id_type=pl.DeviceIdType.MESH,
        )

    fetches = [
        pltpu.make_async_copy(block_hbm, slot(me), local_sem.at[0]),
        pltpu.make_async_copy(q_hbm, q_ref, local_sem.at[1]),
        pltpu.make_async_copy(groups_hbm, groups_ref, local_sem.at[2]),
        pltpu.make_async_copy(lengths_hbm, lengths_ref, local_sem.at[3]),
    ]
    barrier = pltpu.get_barrier_semaphore()
    for fetch in fetches:
        fetch.start()

    @pl.loop(1, members)
    def _(d):
        pl.semaphore_signal(
            barrier, inc=1, device_id={"ref": place(d)}, device_id_type=pl.DeviceIdType.MESH
        )

    fetches[1].wait()

    flip = (
        lax.broadcasted_iota(jnp.int32, (LANES, LANES), 0)
        + lax.broadcasted_iota(jnp.int32, (LANES, LANES), 1)
        == LANES - 1
    ).astype(jnp.bfloat16)
    q_all = q_ref[...].astype(jnp.float32)
    parts = []
    for p in range(per_device):
        pieces = [q_all[p : p + 1, LANES * a : LANES * (a + 1)] for a in range(q_rows)]
        parts += pieces + [jnp.zeros((q_pad - q_rows, LANES), jnp.float32)]
    q_points = jnp.concatenate(parts, axis=0)
    q_scale_ref[...] = window_stats(q_points)[1]
    q_back = jnp.dot(q_points.astype(jnp.bfloat16), flip, preferred_element_type=jnp.float32)
    for p in range(per_device):
        q_base = p * q_pad
        for a in range(full + HALVES):
            tile = toeplitz(
                q_back[q_base + a : q_base + a + 1], q_back[q_base + a + 1 : q_base + a + 2]
            ).astype(jnp.bfloat16)
            for h in range(HALVES):
                if 0 <= a - h < full:
                    left_ref[p, pl.ds((a - h) * LANES, LANES), pl.ds(h * LANES, LANES)] = tile
                elif a - h == full:
                    left_ref[p, pl.ds(full * LANES, 16), pl.ds(h * LANES, LANES)] = tile[:16]
        mean_ref[p] = jnp.dot(
            left_ref[p], jnp.full((M, LANES), 1.0 / M, jnp.bfloat16), preferred_element_type=jnp.float32
        )

    fetches[0].wait()
    pl.semaphore_wait(barrier, members - 1)

    @pl.loop(1, members)
    def _(d):
        copy(d, me).start()

    fetches[2].wait()
    fetches[3].wait()

    @pl.loop(1, members)
    def _(d):
        copy(d, place(members - d)).wait_recv()

    column = lax.broadcasted_iota(jnp.int32, (r_pad, all_rows), 1)
    wanted = lax.broadcasted_iota(jnp.int32, (r_pad, all_rows), 0)
    picks = [
        jnp.where(column == wanted + groups_ref[p] * rows, 1.0, 0.0).astype(jnp.bfloat16)
        for p in range(per_device)
    ]
    points = jnp.dot(
        jnp.concatenate(picks, axis=0), series_ref[...], preferred_element_type=jnp.float32
    )
    total, scale = window_stats(points)
    total_ref[...] = total
    scale_ref[...] = scale

    for p in range(per_device):
        r_base = p * r_pad
        q_base = p * q_pad
        tiles = hankel_tiles([points[r_base + m : r_base + m + 1] for m in range(rows + HALVES)])
        for m, tile in enumerate(tiles):
            right_ref[m] = tile

        g = groups_ref[p]

        def multiply(products_ref, first):
            right = jnp.concatenate(
                [
                    jnp.concatenate([right_ref[first + h + n] for n in range(CHUNK)], axis=1)
                    for h in range(HALVES)
                ],
                axis=0,
            )
            products_ref[...] = jnp.dot(left_ref[p], right, preferred_element_type=jnp.float32)

        def fold(products_ref, first, last):
            totals = [total_ref[pl.ds(r_base + first + n, 1), :] for n in range(CHUNK)]
            scales = [scale_ref[pl.ds(r_base + first + n, 1), :] for n in range(CHUNK)]
            if last:
                lane = lax.broadcasted_iota(jnp.int32, (1, LANES), 1)
                start = (g * rows + first) * LANES
                limit = all_rows * LANES - M
                floors = [
                    jnp.where(start + n * LANES + lane <= limit, 0.0, MASKED) for n in range(CHUNK)
                ]
            for t in range(0, tall, 16):
                mean = mean_ref[p, pl.ds(t, 16), :]
                best = None
                for n in range(CHUNK):
                    piece = products_ref[pl.ds(t, 16), pl.ds(n * LANES, LANES)]
                    value = (piece - mean * totals[n]) * scales[n]
                    if last:
                        value = value + floors[n]
                    best = value if best is None else jnp.maximum(best, value)
                if not last:
                    best = jnp.maximum(best, acc_ref[pl.ds(t, 16), :])
                acc_ref[pl.ds(t, 16), :] = best

        multiply(even_ref, rows - CHUNK)
        multiply(odd_ref, 0)
        fold(even_ref, rows - CHUNK, True)

        @pl.loop(0, rows // (2 * CHUNK) - 1)
        def _(i):
            first = 2 * CHUNK * i
            multiply(even_ref, first + CHUNK)
            fold(odd_ref, first, False)
            multiply(odd_ref, first + 2 * CHUNK)
            fold(even_ref, first + CHUNK, False)

        fold(odd_ref, rows - 2 * CHUNK, False)

        lane = lax.broadcasted_iota(jnp.int32, (1, LANES), 1)
        limit = lengths_ref[p] - M
        for a in range(q_rows):
            if a < full:
                block = acc_ref[pl.ds(a * LANES, LANES), :]
                best = jnp.max(block.T, axis=0, keepdims=True)
            elif a == full:
                block = acc_ref[pl.ds(a * LANES, 8), :]
                best = jnp.broadcast_to(jnp.max(block, axis=1, keepdims=True)[:1], (1, LANES))
            if a <= full:
                best = best * q_scale_ref[pl.ds(q_base + a, 1), :] * (1.0 / M)
                row = jnp.where(a * LANES + lane <= limit, 2.0 * (1.0 - best), 0.0)
            else:
                row = jnp.zeros((1, LANES), jnp.float32)
            out_ref[pl.ds(p, 1), pl.ds(a * LANES, LANES)] = row

    @pl.loop(1, members)
    def _(d):
        copy(d, me).wait_send()


def join(members, groups, lengths, queries, block):
    per_device, series_len = queries.shape
    rows = block.shape[0]
    tall = (series_len - M) // LANES * LANES + 16
    r_rows = per_device * (rows + 16)
    q_rows = per_device * (series_len // LANES + 8)
    vmem = pl.BlockSpec(memory_space=pltpu.VMEM)
    return pl.pallas_call(
        functools.partial(join_kernel, members),
        out_shape=pltpu.VMEM((per_device, series_len), jnp.float32),
        in_specs=[pl.BlockSpec(memory_space=pl.ANY)] * 4,
        out_specs=vmem,
        scratch_shapes=[
            pltpu.VMEM((members * rows, LANES), jnp.bfloat16),
            pltpu.VMEM((per_device, tall, M), jnp.bfloat16),
            pltpu.VMEM((rows + 1, LANES, LANES), jnp.bfloat16),
            pltpu.VMEM((per_device, tall, LANES), jnp.float32),
            pltpu.VMEM((r_rows, LANES), jnp.float32),
            pltpu.VMEM((r_rows, LANES), jnp.float32),
            pltpu.VMEM((q_rows, LANES), jnp.float32),
            pltpu.VMEM((tall, LANES), jnp.float32),
            pltpu.VMEM((tall, CHUNK * LANES), jnp.float32),
            pltpu.VMEM((tall, CHUNK * LANES), jnp.float32),
            pltpu.VMEM((per_device, series_len), jnp.bfloat16),
            pltpu.SMEM((per_device,), jnp.int32),
            pltpu.SMEM((per_device,), jnp.int32),
            pltpu.SemaphoreType.DMA((4,)),
            pltpu.SemaphoreType.DMA((members,)),
            pltpu.SemaphoreType.DMA((members,)),
        ],
        compiler_params=pltpu.CompilerParams(collective_id=0, has_side_effects=True),
        name="join",
    )(groups, lengths, queries, block)


def body(long_series, queries, lengths, groups):
    members = lax.axis_size("ref")
    return join(members, groups, lengths, queries, long_series.reshape(-1, LANES))


def solution(mesh):
    in_specs = (
        P(("groups", "ref")),
        P(("groups", "ref"), None),
        P(("groups", "ref")),
        P(("groups", "ref")),
    )
    out_specs = P(("groups", "ref"), None)
    return jax.shard_map(body, mesh=mesh, in_specs=in_specs, out_specs=out_specs, check_vma=False)
```
